32 devices in a mesh: groups: 2 (over y), gx: 8 (over z, x), gy: 2 (over core).
Axes of the slice: x: 2, y: 2, z: 4, core: 2. Of those that a mesh axis runs over, the one named last changes fastest.
Arguments:
- forcing: float32 [2, 512, 3072], P(None, ('groups', 'gx'), 'gy'), parts along dimension 1, may hold values from -6 to 6
- viscosity: float32 [512, 3072], P(('groups', 'gx'), 'gy'), parts along dimension 0, may hold values from 0.25 to 8
- mass: float32 [512, 3072], P(('groups', 'gx'), 'gy'), parts along dimension 0, may hold values from 0.5 to 2
- coriolis: float32 [3072], P('gy'), may hold values from 0.1 to 0.45
- land: int32 [256, 3072], P('gx', 'gy'), may hold values 0 or 1
- ice_tiles: int32 [4, 24], P('groups'), parts along dimension 0, may hold values 0 or 1
Outputs:
- velocity: float32 [2, 512, 3072], P(None, ('groups', 'gx'), 'gy'), parts along dimension 1
The draws below stay inside these ranges and needn't reach their ends.
There are 2 independent parts, one for each index of `groups`. The reference program is written for one: setup_inputs(seed, part) draws one part's arguments, and reference() takes and returns one part's arrays. A program takes and returns all parts, laid end to end along the dimension named above; an argument that names none is the same for every part. Nothing has to cross between parts.
Inputs may be any that keep to these rules, and one draw needn't show every extreme that they name: 1 marks land. `ice_tiles`: 1 marks a tile with ice.
All inputs are finite; a program needn't handle non-finite values. No bound on the sum of `land` on one device may be relied on, other than what follows from the above.
Results may differ from the reference program's by a relative error of at most 0.00005.
Values sent between devices are 32-bit elements; how exact they have to be, the bound alone decides.
A program may use at most 64 MiB of HBM per device.

```python
import math
import jax
import jax.numpy as jnp

TILE = 128
LEVELS = 4
PRE = 1
POST = 1
CSWEEPS = 3
CYCLES = 1
NX = 256
NY = 3072


def touch_ends(array, own_key, smallest, top_value):
    place = [jax.random.randint(jax.random.fold_in(own_key, axis), (), 0, length) for axis, length in enumerate(array.shape)]
    widest = array.shape.index(max(array.shape))
    beside = place[:widest] + [(place[widest] + 1) % array.shape[widest]] + place[widest + 1:]
    return array.at[tuple(place)].set(smallest).at[tuple(beside)].set(top_value)


def level_of(key, shape, cuts, low, largest):
    gain, own = 1.0, jax.random.fold_in(key, 6)
    for dim, blocks in cuts:
        heights = jnp.exp(jax.random.uniform(jax.random.fold_in(own, dim), (blocks,), jnp.float32, low / len(cuts), largest / len(cuts)))
        gain = gain * jnp.repeat(heights, shape[dim] // blocks).reshape([-1 if axis == dim else 1 for axis in range(len(shape))])
    return gain


def noise(own_key, extent, width, limit, cuts=(), kind=jnp.bfloat16):
    values = width * jax.random.normal(own_key, extent, jnp.float32)
    if cuts:
        values = values * level_of(own_key, extent, cuts, -0.22, 0.18)
    return jnp.clip(values, -limit, limit).astype(kind)


def setup_inputs(seed: int = 0, part: int = 0) -> dict:
    arg_keys = jax.random.split(jax.random.key(seed), 7)
    own_keys = jax.random.split(jax.random.fold_in(arg_keys[6], part), 7)
    forcing = noise(own_keys[0], (2, NX, NY), 1.0, 6.0, ((1, 8), (2, 2)), jnp.float32)
    viscosity = jnp.clip(jnp.exp(math.log(8.0) - 3.465736 * jax.random.uniform(own_keys[1], (NX, NY), jnp.float32) ** level_of(own_keys[1], (NX, NY), ((0, 8), (1, 2)), -0.2, 0.2)), 0.25, 8.0)
    mass = jnp.clip(jnp.exp(math.log(2.0) - 1.3862944 * jax.random.uniform(own_keys[2], (NX, NY), jnp.float32) ** level_of(own_keys[2], (NX, NY), ((0, 8), (1, 2)), -0.2, 0.2)), 0.5, 2.0)
    coriolis = jnp.clip(0.1 + 0.35 * jax.random.uniform(arg_keys[3], (NY,), jnp.float32) ** level_of(arg_keys[3], (NY,), ((0, 2),), -0.2, 0.2), 0.1, 0.45)
    land = touch_ends((jax.random.randint(arg_keys[4], (NX, NY), 0, 6) < 1).astype(jnp.int32), jax.random.fold_in(arg_keys[4], 1), 0, 1)
    ice_tiles = touch_ends((jax.random.randint(own_keys[5], (NX // TILE, NY // TILE), 0, 4) < 3).astype(jnp.int32), jax.random.fold_in(own_keys[5], 1), 0, 1)
    return {"forcing": forcing, "viscosity": viscosity, "mass": mass, "coriolis": coriolis, "land": land, "ice_tiles": ice_tiles}


relax_weight = 0.8
land_mass = 4.0


def pair_mean(values):
    return 0.25 * (values[..., 0::2, 0::2] + values[..., 1::2, 0::2] + values[..., 0::2, 1::2] + values[..., 1::2, 1::2])


def build_levels(visc_eff, mass_eff, coriolis):
    east = 0.5 * (visc_eff + jnp.roll(visc_eff, -1, 0))
    west = jnp.roll(east, 1, 0)
    inner = 0.5 * (visc_eff[:, :-1] + visc_eff[:, 1:])
    folded = 0.5 * (visc_eff[:, -1] + visc_eff[::-1, -1])
    north = jnp.concatenate([inner, folded[:, None]], 1)
    south = jnp.concatenate([visc_eff[:, :1], north[:, :-1]], 1)
    mass_now = mass_eff
    rotation = coriolis
    levels = []
    for level in range(LEVELS):
        if level > 0:
            east = 0.25 * (east[1::2, 0::2] + east[1::2, 1::2])
            west = 0.25 * (west[0::2, 0::2] + west[0::2, 1::2])
            north = 0.25 * (north[0::2, 1::2] + north[1::2, 1::2])
            south = 0.25 * (south[0::2, 0::2] + south[1::2, 0::2])
            mass_now = pair_mean(mass_now)
            rotation = 0.5 * (rotation[0::2] + rotation[1::2])
        diagonal = mass_now + east + west + north + south
        levels.append((east, west, north, south, diagonal, rotation))
    return levels


def apply_operator(field, stencil):
    east, west, north, south, diagonal, rotation = stencil
    east_nb = jnp.roll(field, -1, 1)
    west_nb = jnp.roll(field, 1, 1)
    north_nb = jnp.concatenate([field[:, :, 1:], -field[:, ::-1, -1:]], 2)
    south_nb = jnp.concatenate([jnp.zeros_like(field[:, :, :1]), field[:, :, :-1]], 2)
    turned = jnp.stack([-field[1], field[0]]) * rotation
    return diagonal * field - east * east_nb - west * west_nb - north * north_nb - south * south_nb + turned


def smooth(field, source, stencil, count, from_zero):
    for sweep in range(count):
        if from_zero and sweep == 0:
            field = relax_weight * source / stencil[4]
        else:
            field = field + relax_weight * (source - apply_operator(field, stencil)) / stencil[4]
    return field


def vcycle(level, source, field, from_zero, levels):
    stencil = levels[level]
    if level == LEVELS - 1:
        return smooth(field, source, stencil, CSWEEPS, True)
    field = smooth(field, source, stencil, PRE, from_zero)
    residue = source - apply_operator(field, stencil)
    coarse = vcycle(level + 1, pair_mean(residue), None, True, levels)
    field = field + jnp.repeat(jnp.repeat(coarse, 2, 1), 2, 2)
    return smooth(field, source, stencil, POST, False)


def reference(forcing, viscosity, mass, coriolis, land, ice_tiles):
    land_float = land.astype(jnp.float32)
    ocean = 1.0 - land_float
    ice = jnp.repeat(jnp.repeat(ice_tiles.astype(jnp.float32), TILE, 0), TILE, 1)
    visc_eff = viscosity * ice * ocean
    mass_eff = mass * ocean + land_mass * land_float
    source = forcing * ocean
    levels = build_levels(visc_eff, mass_eff, coriolis)
    field = None
    for cycle in range(CYCLES):
        field = vcycle(0, source, field, cycle == 0, levels)
    return field
```

```python
import functools

import jax
import jax.numpy as jnp
from jax import lax
from jax.experimental import pallas as pl
from jax.experimental.pallas import tpu as pltpu
from jax.sharding import PartitionSpec as P

TILE = 128
LANES = 128
HALF = 64
HX = 8
COMP = 4
RELAX = 0.8
LAND_MASS = 4.0
MESH = pl.DeviceIdType.MESH
HIGH = lax.Precision.HIGHEST


def iota(shape, dim):
    return lax.broadcasted_iota(jnp.int32, shape, dim)


def dot(a, b):
    return jnp.dot(a, b, precision=HIGH, preferred_element_type=jnp.float32)


def shift(x, step, dim):
    size = x.shape[dim]
    return pltpu.roll(x, (-step) % size, dim)


def pair_sum(x, dim, step):
    odd = (iota(x.shape, dim) // step) % 2 == 1
    return x + jnp.where(odd, shift(x, -step, dim), shift(x, step, dim))


def odd_of_pair(x, dim, step):
    odd = (iota(x.shape, dim) // step) % 2 == 1
    return jnp.where(odd, x, shift(x, step, dim))


def coarsen(east, north, mass, rot, step):
    east = 0.25 * pair_sum(odd_of_pair(east, 0, step), 1, step)
    north = 0.25 * pair_sum(odd_of_pair(north, 1, step), 0, step)
    mass = 0.25 * pair_sum(pair_sum(mass, 0, step), 1, step)
    rot = 0.5 * pair_sum(rot, 1, step)
    return east, north, mass, rot


def stencil_of(east, north, mass, rot, keep, step):
    west = shift(east, -step, 0)
    south = shift(north, -step, 1)
    diag = mass + east + west + north + south
    return east, west, north, south, diag, keep * (RELAX / diag), rot


def off_diagonal(w, st, step):
    east, west, north, south, _, _, rot = st
    out = []
    for c in range(2):
        turned = -w[1] if c == 0 else w[0]
        out.append(
            east * shift(w[c], step, 0)
            + west * shift(w[c], -step, 0)
            + north * shift(w[c], step, 1)
            + south * shift(w[c], -step, 1)
            - rot * turned
        )
    return out


def from_zero(b, st):
    return [st[5] * b[c] for c in range(2)]


def residual_from_zero(b, w, st, step):
    off = off_diagonal(w, st, step)
    return [(1.0 - RELAX) * b[c] + off[c] for c in range(2)]


def sweep(w, b, st, step):
    off = off_diagonal(w, st, step)
    return [w[c] + st[5] * (b[c] - st[4] * w[c] + off[c]) for c in range(2)]


def restrict(r, step):
    return [0.25 * pair_sum(pair_sum(r[c], 0, step), 1, step) for c in range(2)]


def halo_place(k):
    return jnp.where(k < HALF, k // COMP, k // COMP + LANES - LANES // COMP)


def compact(x, own, select):
    block = COMP * LANES
    row, col = iota((block, LANES), 0), iota((block, LANES), 1)
    hit = (row == COMP * col + COMP - 1) if select else (row // COMP == col)
    m = jnp.where(hit, 1.0 / COMP, 0.0)
    row, col = iota((LANES, LANES), 0), iota((LANES, LANES), 1)
    hit = halo_place(row) == col
    if select:
        hit = hit & (row % COMP == COMP - 1)
    mh = jnp.where(hit, 1.0 / COMP, 0.0)
    parts = [
        dot(x[:, k * block : (k + 1) * block], m)
        for k in range(own // block)
    ]
    parts.append(dot(x[:, own:], mh))
    return jnp.concatenate(parts, 1)


def expand(x, own):
    block = COMP * LANES
    row, col = iota((LANES, block), 0), iota((LANES, block), 1)
    m = jnp.where(row == col // COMP, 1.0, 0.0)
    row, col = iota((LANES, LANES), 0), iota((LANES, LANES), 1)
    mh = jnp.where(row == halo_place(col), 1.0, 0.0)
    count = own // block
    parts = [
        dot(x[:, k * LANES : (k + 1) * LANES], m)
        for k in range(count)
    ]
    parts.append(dot(x[:, count * LANES :], mh))
    return jnp.concatenate(parts, 1)


def kernel(
    gx, gy, f_ref, v_ref, m_ref, cor_ref, land_ref, ice_ref, out_ref,
    ext, from_n, from_s, lev2, send, recv,
):
    nx, ny = v_ref.shape
    full = ny + LANES
    grp = lax.axis_index("groups")
    g = lax.axis_index("gx")
    r = lax.axis_index("gy")
    at_top = r == gy - 1
    at_bottom = r == 0
    right = (grp, lax.rem(g + 1, gx), r)
    left = (grp, lax.rem(g + gx - 1, gx), r)
    above = (grp, g, r + 1)
    below = (grp, g, r - 1)
    mirror = (grp, gx - 1 - g, r)

    barrier = pltpu.get_barrier_semaphore()

    def hello(device):
        pl.semaphore_signal(barrier, inc=1, device_id=device, device_id_type=MESH)

    hello(right)
    hello(left)

    @pl.when(at_top)
    def _():
        hello(mirror)

    @pl.when(jnp.logical_not(at_top))
    def _():
        hello(above)

    @pl.when(jnp.logical_not(at_bottom))
    def _():
        hello(below)

    land = land_ref[...].astype(jnp.float32)
    ocean = 1.0 - land
    tiles_x, tiles_y = ice_ref.shape
    ice_f = ice_ref[...].astype(jnp.float32)
    tile_row = (g * nx + iota((nx, tiles_y), 0)) // TILE
    ice_rows = jnp.zeros((nx, tiles_y), jnp.float32)
    for t in range(tiles_x):
        ice_rows = ice_rows + jnp.where(tile_row == t, ice_f[t : t + 1, :], 0.0)
    pick = jnp.where((r * ny + iota((tiles_y, ny), 1)) // TILE == iota((tiles_y, ny), 0), 1.0, 0.0)
    ice = jnp.dot(ice_rows, pick, preferred_element_type=jnp.float32)
    ext[0, 0:nx, 0:ny] = v_ref[...] * ice * ocean
    ext[1, 0:nx, 0:ny] = m_ref[...] * ocean + LAND_MASS * land
    ext[2, 0:nx, 0:ny] = f_ref[0] * ocean
    ext[3, 0:nx, 0:ny] = f_ref[1] * ocean
    ext[4, 0:nx, 0:ny] = jnp.broadcast_to(cor_ref[...], (nx, ny))

    pl.semaphore_wait(barrier, jnp.where(at_bottom, 3, 4))

    def copy(src, dst, k, device):
        return pltpu.make_async_remote_copy(
            src_ref=src, dst_ref=dst, send_sem=send.at[k], recv_sem=recv.at[k],
            device_id=device, device_id_type=MESH,
        )

    top_tile = ext.at[:, 0:nx, ny - LANES : ny]
    low_tile = ext.at[:, 0:nx, 0:LANES]
    to_mirror = copy(top_tile, from_n, 0, mirror)
    to_below = copy(low_tile, from_n, 2, below)
    to_above = copy(top_tile, from_s, 1, above)

    @pl.when(at_top)
    def _():
        to_mirror.start()

    @pl.when(jnp.logical_not(at_top))
    def _():
        to_above.start()

    @pl.when(jnp.logical_not(at_bottom))
    def _():
        to_below.start()

    def x_copy(buf, k, lo, hi, size, width, count):
        return (
            copy(buf.at[0:count, size - width : size, lo:hi],
                 buf.at[0:count, size + width : size + 2 * width, lo:hi], k, right),
            copy(buf.at[0:count, 0:width, lo:hi],
                 buf.at[0:count, size : size + width, lo:hi], k + 1, left),
        )

    bulk = x_copy(ext, 3, 0, ny, nx, HX, 4)
    for c in bulk:
        c.start()

    @pl.when(at_top)
    def _():
        to_mirror.wait()
        row, col = iota((LANES, LANES), 0), iota((LANES, LANES), 1)
        flip_l = jnp.where(row + col == LANES - 1, 1.0, 0.0)
        row, col = iota((nx, nx), 0), iota((nx, nx), 1)
        flip_r = jnp.where(row + col == nx - 1, 1.0, 0.0)
        for f in range(5):
            sign = -1.0 if f in (2, 3) else 1.0
            t = dot(from_n[f], flip_l)
            t = dot(sign * flip_r, t)
            ext[f, 0:nx, ny:full] = t

    @pl.when(jnp.logical_not(at_top))
    def _():
        to_above.wait_send()
        to_below.wait_recv()
        ext[:, 0:nx, ny:full] = from_n[...]

    south_part = iota((nx, LANES), 1) >= HALF

    @pl.when(at_bottom)
    def _():
        for f in range(5):
            if f == 0:
                fill = jnp.broadcast_to(ext[0, 0:nx, 0:1], (nx, LANES))
            else:
                fill = jnp.full((nx, LANES), 1.0 if f == 1 else 0.0, jnp.float32)
            ext[f, 0:nx, ny:full] = jnp.where(south_part, fill, ext[f, 0:nx, ny:full])

    @pl.when(jnp.logical_not(at_bottom))
    def _():
        to_below.wait_send()
        to_above.wait_recv()
        for f in range(5):
            ext[f, 0:nx, ny:full] = jnp.where(south_part, from_s[f], ext[f, 0:nx, ny:full])

    corner = x_copy(ext, 5, ny, full, nx, HX, 4)
    for c in corner:
        c.start()
    for c in bulk:
        c.wait()
    for c in corner:
        c.wait()

    visc, mass = ext[0], ext[1]
    src = [ext[2], ext[3]]
    rot = ext[4, 0:8]
    lane = iota((1, full), 1)
    keep = jnp.where((lane >= ny + HALF) & at_bottom, 0.0, 1.0)
    east = 0.5 * (visc + shift(visc, 1, 0))
    north = 0.5 * (visc + shift(visc, 1, 1))
    st0 = stencil_of(east, north, mass, rot[0:1], keep, 1)
    w0 = from_zero(src, st0)
    b1 = restrict(residual_from_zero(src, w0, st0, 1), 1)
    east1, north1, mass1, rot1 = coarsen(east, north, mass, rot, 1)
    st1 = stencil_of(east1, north1, mass1, rot1[0:1], keep, 2)
    w1 = from_zero(b1, st1)
    r1 = residual_from_zero(b1, w1, st1, 2)
    cx = nx // COMP
    row, col = iota((cx, nx), 0), iota((cx, nx), 1)
    mean_rows = jnp.where(col // COMP == row, 1.0 / COMP, 0.0)
    last_rows = jnp.where(col == COMP * row + COMP - 1, 1.0 / COMP, 0.0)
    avg = compact(jnp.concatenate([r1[0][0:nx], r1[1][0:nx], mass[0:nx], east[0:nx], rot], 0), ny, False)
    sel = compact(north[0:nx], ny, True)
    for k in range(4):
        lev2[k, 0:cx] = dot(last_rows if k == 3 else mean_rows, avg[k * nx : (k + 1) * nx])
    lev2[4, 0:cx] = dot(mean_rows, sel)
    rot2 = avg[4 * nx : 4 * nx + 8]
    third = x_copy(lev2, 7, 0, lev2.shape[2], cx, cx, 5)
    for c in third:
        c.start()
    for c in third:
        c.wait()
    b2 = [lev2[0], lev2[1]]
    mass2, east2, north2 = lev2[2], lev2[3], lev2[4]
    full2 = lev2.shape[2]
    lane2 = iota((1, full2), 1)
    used = (lane2 < ny // COMP + HALF // COMP) | (lane2 >= full2 - HALF // COMP)
    below2 = (lane2 >= full2 - HALF // COMP) & at_bottom
    keep2 = jnp.where(used & jnp.logical_not(below2), 1.0, 0.0)
    mass2 = jnp.where(used, mass2, 1.0)
    st2 = stencil_of(east2, north2, mass2, rot2[0:1], keep2, 1)
    w2 = from_zero(b2, st2)
    b3 = restrict(residual_from_zero(b2, w2, st2, 1), 1)
    east3, north3, mass3, rot3 = coarsen(east2, north2, mass2, rot2, 1)
    st3 = stencil_of(east3, north3, mass3, rot3[0:1], keep2, 2)
    e3 = from_zero(b3, st3)
    e3 = sweep(e3, b3, st3, 2)
    e3 = sweep(e3, b3, st3, 2)
    w2 = sweep([w2[c] + e3[c] for c in range(2)], b2, st2, 1)
    row, col = iota((nx + 2 * HX, 3 * cx), 0), iota((nx + 2 * HX, 3 * cx), 1)
    from_row = jnp.where(row < nx + HX, row // COMP, row // COMP + 3 * cx - (nx + 2 * HX) // COMP)
    spread = jnp.where(from_row == col, 1.0, 0.0)
    up = expand(jnp.concatenate([dot(spread, w2[c]) for c in range(2)], 0), ny)
    up = [up[0 : nx + 2 * HX], up[nx + 2 * HX :]]
    e1 = sweep([w1[c] + up[c] for c in range(2)], b1, st1, 2)
    w0 = sweep([w0[c] + e1[c] for c in range(2)], src, st0, 1)
    for c in range(2):
        out_ref[c] = w0[c][0:nx, 0:ny]


def local(gx, gy, forcing, viscosity, mass, coriolis, land, ice_tiles):
    nx, ny = viscosity.shape
    ext = (nx + 2 * HX, ny + LANES)
    return pl.pallas_call(
        functools.partial(kernel, gx, gy),
        out_shape=jax.ShapeDtypeStruct(forcing.shape, jnp.float32),
        in_specs=[pl.BlockSpec(memory_space=pltpu.VMEM)] * 6,
        out_specs=pl.BlockSpec(memory_space=pltpu.VMEM),
        scratch_shapes=[
            pltpu.VMEM((5,) + ext, jnp.float32),
            pltpu.VMEM((5, nx, LANES), jnp.float32),
            pltpu.VMEM((5, nx, LANES), jnp.float32),
            pltpu.VMEM((5, 3 * (nx // COMP), ny // COMP + LANES), jnp.float32),
            pltpu.SemaphoreType.DMA((9,)),
            pltpu.SemaphoreType.DMA((9,)),
        ],
        compiler_params=pltpu.CompilerParams(collective_id=0, has_side_effects=True),
    )(forcing, viscosity, mass, coriolis.reshape(1, -1), land, ice_tiles)


def solution(mesh):
    return jax.shard_map(
        functools.partial(local, mesh.shape["gx"], mesh.shape["gy"]),
        mesh=mesh,
        in_specs=(
            P(None, ("groups", "gx"), "gy"),
            P(("groups", "gx"), "gy"),
            P(("groups", "gx"), "gy"),
            P("gy"),
            P("gx", "gy"),
            P("groups", None),
        ),
        out_specs=P(None, ("groups", "gx"), "gy"),
        check_vma=False,
    )
```

```python
import functools

import jax
import jax.numpy as jnp
from jax import lax
from jax.experimental import pallas as pl
from jax.experimental.pallas import tpu as pltpu
from jax.sharding import PartitionSpec as P

TILE = 128
LANES = 128
HALF = 32
HX = 8
COMP = 4
RELAX = 0.8
LAND_MASS = 4.0
MESH = pl.DeviceIdType.MESH
HIGH = lax.Precision.HIGHEST


def iota(shape, dim):
    return lax.broadcasted_iota(jnp.int32, shape, dim)


def dot(a, b):
    return jnp.dot(a, b, precision=HIGH, preferred_element_type=jnp.float32)


def shift(x, step, dim):
    size = x.shape[dim]
    return pltpu.roll(x, (-step) % size, dim)


def pair_sum(x, dim, step):
    odd = (iota(x.shape, dim) // step) % 2 == 1
    return x + jnp.where(odd, shift(x, -step, dim), shift(x, step, dim))


def odd_of_pair(x, dim, step):
    odd = (iota(x.shape, dim) // step) % 2 == 1
    return jnp.where(odd, x, shift(x, step, dim))


def coarsen(east, north, mass, rot, step):
    east = 0.25 * pair_sum(odd_of_pair(east, 0, step), 1, step)
    north = 0.25 * pair_sum(odd_of_pair(north, 1, step), 0, step)
    mass = 0.25 * pair_sum(pair_sum(mass, 0, step), 1, step)
    rot = 0.5 * pair_sum(rot, 1, step)
    return east, north, mass, rot


def stencil_of(east, north, mass, rot, keep, step):
    west = shift(east, -step, 0)
    south = shift(north, -step, 1)
    diag = mass + east + west + north + south
    return east, west, north, south, diag, keep * (RELAX / diag), rot


def off_diagonal(w, st, step):
    east, west, north, south, _, _, rot = st
    out = []
    for c in range(2):
        turned = -w[1] if c == 0 else w[0]
        out.append(
            east * shift(w[c], step, 0)
            + west * shift(w[c], -step, 0)
            + north * shift(w[c], step, 1)
            + south * shift(w[c], -step, 1)
            - rot * turned
        )
    return out


def from_zero(b, st):
    return [st[5] * b[c] for c in range(2)]


def residual_from_zero(b, w, st, step):
    off = off_diagonal(w, st, step)
    return [(1.0 - RELAX) * b[c] + off[c] for c in range(2)]


def sweep(w, b, st, step):
    off = off_diagonal(w, st, step)
    return [w[c] + st[5] * (b[c] - st[4] * w[c] + off[c]) for c in range(2)]


def restrict(r, step):
    return [0.25 * pair_sum(pair_sum(r[c], 0, step), 1, step) for c in range(2)]


def halo_place(k):
    return jnp.where(k < HALF, k // COMP, k // COMP + LANES - LANES // COMP)


def compact(x, own, select):
    block = COMP * LANES
    row, col = iota((block, LANES), 0), iota((block, LANES), 1)
    hit = (row == COMP * col + COMP - 1) if select else (row // COMP == col)
    m = jnp.where(hit, 1.0 / COMP, 0.0)
    row, col = iota((LANES, LANES), 0), iota((LANES, LANES), 1)
    hit = halo_place(row) == col
    if select:
        hit = hit & (row % COMP == COMP - 1)
    mh = jnp.where(hit, 1.0 / COMP, 0.0)
    parts = [
        dot(x[:, k * block : (k + 1) * block], m)
        for k in range(own // block)
    ]
    parts.append(dot(x[:, own:], mh))
    return jnp.concatenate(parts, 1)


def expand(x, own):
    block = COMP * LANES
    row, col = iota((LANES, block), 0), iota((LANES, block), 1)
    m = jnp.where(row == col // COMP, 1.0, 0.0)
    row, col = iota((LANES, LANES), 0), iota((LANES, LANES), 1)
    mh = jnp.where(row == halo_place(col), 1.0, 0.0)
    count = own // block
    parts = [
        dot(x[:, k * LANES : (k + 1) * LANES], m)
        for k in range(count)
    ]
    parts.append(dot(x[:, count * LANES :], mh))
    return jnp.concatenate(parts, 1)


DEPTH = (6, 5, 5, 5)
FILL = (0.0, 1.0, 0.0, 0.0)


def edges():
    offset, out = 0, []
    for depth in DEPTH:
        out.append((offset, depth))
        offset += depth
    return out


def kernel(
    gx, gy, f_hbm, v_hbm, m_hbm, cor_ref, land_hbm, ice_ref, out_ref,
    f_ref, v_ref, m_ref, land_ref, ext, rotx, low_pack, top_pack, from_n, from_s,
    to_r, to_l, from_r, from_l, lev2, load, send, recv,
):
    nx, ny = v_ref.shape
    full = ny + LANES
    grp = lax.axis_index("groups")
    g = lax.axis_index("gx")
    r = lax.axis_index("gy")
    at_top = r == gy - 1
    at_bottom = r == 0
    not_top = jnp.logical_not(at_top)
    not_bottom = jnp.logical_not(at_bottom)
    right = (grp, lax.rem(g + 1, gx), r)
    left = (grp, lax.rem(g + gx - 1, gx), r)
    above = (grp, g, r + 1)
    below = (grp, g, r - 1)
    mirror = (grp, gx - 1 - g, r)

    barrier = pltpu.get_barrier_semaphore()

    def hello(device):
        pl.semaphore_signal(barrier, inc=1, device_id=device, device_id_type=MESH)

    @pl.when(at_top)
    def _():
        hello(mirror)

    hello(right)
    hello(left)

    @pl.when(not_top)
    def _():
        hello(above)

    @pl.when(not_bottom)
    def _():
        hello(below)

    loads = [
        pltpu.make_async_copy(a, b, load.at[k])
        for k, (a, b) in enumerate(((land_hbm, land_ref), (v_hbm, v_ref), (m_hbm, m_ref), (f_hbm, f_ref)))
    ]
    for c in loads:
        c.start()
    tiles_x, tiles_y = ice_ref.shape
    ice_f = ice_ref[...].astype(jnp.float32)
    tile_row = (g * nx + iota((nx, tiles_y), 0)) // TILE
    ice_rows = jnp.zeros((nx, tiles_y), jnp.float32)
    for t in range(tiles_x):
        ice_rows = ice_rows + jnp.where(tile_row == t, ice_f[t : t + 1, :], 0.0)
    pick = jnp.where((r * ny + iota((tiles_y, ny), 1)) // TILE == iota((tiles_y, ny), 0), 1.0, 0.0)
    ice = jnp.dot(ice_rows, pick, preferred_element_type=jnp.float32)
    rotx[:, 0:ny] = jnp.broadcast_to(cor_ref[...].reshape(1, ny), (8, ny))
    for f in range(4):
        ext[f, nx:, :] = jnp.full((2 * HX, full), FILL[f], jnp.float32)
    for c in loads:
        c.wait()
    land = land_ref[...].astype(jnp.float32)
    ocean = 1.0 - land
    ext[0, 0:nx, 0:ny] = v_ref[...] * ice * ocean
    ext[1, 0:nx, 0:ny] = m_ref[...] * ocean + LAND_MASS * land
    ext[2, 0:nx, 0:ny] = f_ref[0] * ocean
    ext[3, 0:nx, 0:ny] = f_ref[1] * ocean

    group = iota((nx, LANES), 1) // HALF
    low, top = jnp.zeros((nx, LANES), jnp.float32), jnp.zeros((nx, LANES), jnp.float32)
    for f in range(4):
        low = jnp.where(group == f, pltpu.roll(ext[f, 0:nx, 0:LANES], HALF * f, 1), low)
        top = jnp.where(
            group == f, pltpu.roll(ext[f, 0:nx, ny - LANES : ny], (HALF * (f + 1)) % LANES, 1), top)
    low_pack[0:nx] = low
    low_pack[nx:] = rotx[:, 0:LANES]
    top_pack[0:nx] = top
    top_pack[nx:] = pltpu.roll(rotx[:, ny - LANES : ny], HALF, 1)

    for f, (o, d) in enumerate(edges()):
        to_r[o : o + d, 0:ny] = ext[f, nx - d : nx, 0:ny]
        to_l[o : o + d, 0:ny] = ext[f, 0:d, 0:ny]

    pl.semaphore_wait(barrier, jnp.where(at_bottom, 3, 4))

    def copy(src, dst, k, device):
        return pltpu.make_async_remote_copy(
            src_ref=src, dst_ref=dst, send_sem=send.at[k], recv_sem=recv.at[k],
            device_id=device, device_id_type=MESH,
        )

    to_mirror = copy(top_pack, from_n, 0, mirror)
    to_above = copy(top_pack, from_s, 1, above)
    to_below = copy(low_pack, from_n, 2, below)

    @pl.when(at_top)
    def _():
        to_mirror.start()

    @pl.when(not_top)
    def _():
        to_above.start()

    @pl.when(not_bottom)
    def _():
        to_below.start()

    def strips(k, lo, hi):
        return (
            copy(to_r.at[:, lo:hi], from_l.at[:, lo:hi], k, right),
            copy(to_l.at[:, lo:hi], from_r.at[:, lo:hi], k + 1, left),
        )

    bulk = strips(3, 0, ny)
    for c in bulk:
        c.start()

    @pl.when(at_top)
    def _():
        to_mirror.wait()
        row, col = iota((LANES, LANES), 0), iota((LANES, LANES), 1)
        flip_l = jnp.where((row // HALF == col // HALF) & (row % HALF + col % HALF == HALF - 1), 1.0, 0.0)
        row, col = iota((nx, nx), 0), iota((nx, nx), 1)
        flip_r = jnp.where(row + col == nx - 1, 1.0, 0.0)
        t = dot(from_n[...], flip_l)
        from_n[0:nx] = dot(flip_r, t[0:nx]) * jnp.where(group >= 2, -1.0, 1.0)
        from_n[nx:] = t[nx:]

    @pl.when(not_top)
    def _():
        to_above.wait_send()
        to_below.wait_recv()

    @pl.when(not_bottom)
    def _():
        to_below.wait_send()
        to_above.wait_recv()

    @pl.when(at_bottom)
    def _():
        from_s[...] = jnp.zeros(from_s.shape, jnp.float32)
        from_s[0:nx] = jnp.where(
            group == 0, jnp.broadcast_to(ext[0, 0:nx, 0:1], (nx, LANES)), jnp.where(group == 1, 1.0, 0.0))

    for f in range(4):
        n = pltpu.roll(from_n[0:nx], (LANES - HALF * f) % LANES, 1)
        s = pltpu.roll(from_s[0:nx], (LANES - HALF * (f + 1)) % LANES, 1)
        ext[f, 0:nx, ny:full] = jnp.where(group == 0, n, jnp.where(group == LANES // HALF - 1, s, FILL[f]))
    group8 = iota((8, LANES), 1) // HALF
    rotx[:, ny:full] = jnp.where(group8 == 0, from_n[nx:], pltpu.roll(from_s[nx:], LANES - HALF, 1))
    for f, (o, d) in enumerate(edges()):
        to_r[o : o + d, ny:full] = ext[f, nx - d : nx, ny:full]
        to_l[o : o + d, ny:full] = ext[f, 0:d, ny:full]

    corner = strips(5, ny, full)
    for c in corner:
        c.start()
    for c in bulk:
        c.wait()
    for c in corner:
        c.wait()
    for f, (o, d) in enumerate(edges()):
        ext[f, nx : nx + d] = from_r[o : o + d]
        ext[f, nx + 2 * HX - d : nx + 2 * HX] = from_l[o : o + d]

    visc, mass = ext[0], ext[1]
    src = [ext[2], ext[3]]
    rot = rotx[...]
    lane = iota((1, full), 1)
    used = (lane < ny + HALF) | ((lane >= full - HALF) & not_bottom)
    keep = jnp.where(used, 1.0, 0.0)
    east = 0.5 * (visc + shift(visc, 1, 0))
    north = 0.5 * (visc + shift(visc, 1, 1))
    cx = nx // COMP
    row, col = iota((cx, nx), 0), iota((cx, nx), 1)
    mean_rows = jnp.where(col // COMP == row, 1.0 / COMP, 0.0)
    last_rows = jnp.where(col == COMP * row + COMP - 1, 1.0 / COMP, 0.0)
    avg = compact(jnp.concatenate([mass[0:nx], east[0:nx], rot], 0), ny, False)
    lev2[2, 0:cx] = dot(mean_rows, avg[0:nx])
    lev2[3, 0:cx] = dot(last_rows, avg[nx : 2 * nx])
    lev2[4, 0:cx] = dot(mean_rows, compact(north[0:nx], ny, True))
    rot2 = avg[2 * nx : 2 * nx + 8]

    def blocks(k, lo, hi):
        return (
            copy(lev2.at[lo:hi, 0:cx], lev2.at[lo:hi, 2 * cx : 3 * cx], k, right),
            copy(lev2.at[lo:hi, 0:cx], lev2.at[lo:hi, cx : 2 * cx], k + 1, left),
        )

    first = blocks(7, 2, 5)
    for c in first:
        c.start()
    st0 = stencil_of(east, north, mass, rot[0:1], keep, 1)
    w0 = from_zero(src, st0)
    b1 = restrict(residual_from_zero(src, w0, st0, 1), 1)
    east1, north1, mass1, rot1 = coarsen(east, north, mass, rot, 1)
    st1 = stencil_of(east1, north1, mass1, rot1[0:1], keep, 2)
    w1 = from_zero(b1, st1)
    r1 = residual_from_zero(b1, w1, st1, 2)
    avg = compact(jnp.concatenate([r1[0][0:nx], r1[1][0:nx]], 0), ny, False)
    for k in range(2):
        lev2[k, 0:cx] = dot(mean_rows, avg[k * nx : (k + 1) * nx])
    second = blocks(9, 0, 2)
    for c in second:
        c.start()
    for c in first:
        c.wait()
    for c in second:
        c.wait()
    b2 = [lev2[0], lev2[1]]
    mass2, east2, north2 = lev2[2], lev2[3], lev2[4]
    full2 = lev2.shape[2]
    lane2 = iota((1, full2), 1)
    used = (lane2 < ny // COMP + HALF // COMP) | (lane2 >= full2 - HALF // COMP)
    below2 = (lane2 >= full2 - HALF // COMP) & at_bottom
    keep2 = jnp.where(used & jnp.logical_not(below2), 1.0, 0.0)
    mass2 = jnp.where(used, mass2, 1.0)
    st2 = stencil_of(east2, north2, mass2, rot2[0:1], keep2, 1)
    w2 = from_zero(b2, st2)
    b3 = restrict(residual_from_zero(b2, w2, st2, 1), 1)
    east3, north3, mass3, rot3 = coarsen(east2, north2, mass2, rot2, 1)
    st3 = stencil_of(east3, north3, mass3, rot3[0:1], keep2, 2)
    e3 = from_zero(b3, st3)
    e3 = sweep(e3, b3, st3, 2)
    e3 = sweep(e3, b3, st3, 2)
    w2 = sweep([w2[c] + e3[c] for c in range(2)], b2, st2, 1)
    row, col = iota((nx + 2 * HX, 3 * cx), 0), iota((nx + 2 * HX, 3 * cx), 1)
    from_row = jnp.where(row < nx + HX, row // COMP, row // COMP + 3 * cx - (nx + 2 * HX) // COMP)
    spread = jnp.where(from_row == col, 1.0, 0.0)
    up = expand(jnp.concatenate([dot(spread, w2[c]) for c in range(2)], 0), ny)
    up = [up[0 : nx + 2 * HX], up[nx + 2 * HX :]]
    e1 = sweep([w1[c] + up[c] for c in range(2)], b1, st1, 2)
    w0 = sweep([w0[c] + e1[c] for c in range(2)], src, st0, 1)
    for c in range(2):
        out_ref[c] = w0[c][0:nx, 0:ny]


def local(gx, gy, forcing, viscosity, mass, coriolis, land, ice_tiles):
    nx, ny = viscosity.shape
    ext = (nx + 2 * HX, ny + LANES)
    strip = pltpu.VMEM((nx + 8, LANES), jnp.float32)
    height = -(-sum(DEPTH) // 8) * 8
    side = pltpu.VMEM((height, ny + LANES), jnp.float32)
    anyspace = pl.BlockSpec(memory_space=pl.ANY)
    vmem = pl.BlockSpec(memory_space=pltpu.VMEM)
    return pl.pallas_call(
        functools.partial(kernel, gx, gy),
        out_shape=jax.ShapeDtypeStruct(forcing.shape, jnp.float32),
        in_specs=[anyspace, anyspace, anyspace, vmem, anyspace, vmem],
        out_specs=vmem,
        scratch_shapes=[
            pltpu.VMEM(forcing.shape, jnp.float32),
            pltpu.VMEM((nx, ny), jnp.float32),
            pltpu.VMEM((nx, ny), jnp.float32),
            pltpu.VMEM((nx, ny), jnp.int32),
            pltpu.VMEM((4,) + ext, jnp.float32),
            pltpu.VMEM((8, ny + LANES), jnp.float32),
            strip, strip, strip, strip,
            side, side, side, side,
            pltpu.VMEM((5, 3 * (nx // COMP), ny // COMP + LANES), jnp.float32),
            pltpu.SemaphoreType.DMA((4,)),
            pltpu.SemaphoreType.DMA((11,)),
            pltpu.SemaphoreType.DMA((11,)),
        ],
        compiler_params=pltpu.CompilerParams(collective_id=0, has_side_effects=True),
    )(forcing, viscosity, mass, coriolis, land, ice_tiles)


def solution(mesh):
    return jax.shard_map(
        functools.partial(local, mesh.shape["gx"], mesh.shape["gy"]),
        mesh=mesh,
        in_specs=(
            P(None, ("groups", "gx"), "gy"),
            P(("groups", "gx"), "gy"),
            P(("groups", "gx"), "gy"),
            P("gy"),
            P("gx", "gy"),
            P("groups", None),
        ),
        out_specs=P(None, ("groups", "gx"), "gy"),
        check_vma=False,
    )
```

```python
import functools

import jax
import jax.numpy as jnp
from jax import lax
from jax.experimental import pallas as pl
from jax.experimental.pallas import tpu as pltpu
from jax.sharding import PartitionSpec as P

TILE = 128
LANES = 128
HALF = 32
HX = 8
COMP = 4
RELAX = 0.8
LAND_MASS = 4.0
MESH = pl.DeviceIdType.MESH


def iota(shape, dim):
    return lax.broadcasted_iota(jnp.int32, shape, dim)


def parts(x):
    high = x.astype(jnp.bfloat16)
    rest = x - high.astype(jnp.float32)
    middle = rest.astype(jnp.bfloat16)
    low = (rest - middle.astype(jnp.float32)).astype(jnp.bfloat16)
    return high, middle, low


def pick_right(x, m):
    m = m.astype(jnp.bfloat16)
    return sum(jnp.dot(p, m, preferred_element_type=jnp.float32) for p in parts(x))


def pick_left(m, x):
    m = m.astype(jnp.bfloat16)
    return sum(jnp.dot(m, p, preferred_element_type=jnp.float32) for p in parts(x))


def shift(x, step, dim):
    size = x.shape[dim]
    return pltpu.roll(x, (-step) % size, dim)


def pair_sum(x, dim, step):
    odd = (iota(x.shape, dim) // step) % 2 == 1
    return x + jnp.where(odd, shift(x, -step, dim), shift(x, step, dim))


def odd_of_pair(x, dim, step):
    odd = (iota(x.shape, dim) // step) % 2 == 1
    return jnp.where(odd, x, shift(x, step, dim))


def coarsen(east, north, mass, rot, step):
    east = 0.25 * pair_sum(odd_of_pair(east, 0, step), 1, step)
    north = 0.25 * pair_sum(odd_of_pair(north, 1, step), 0, step)
    mass = 0.25 * pair_sum(pair_sum(mass, 0, step), 1, step)
    rot = 0.5 * pair_sum(rot, 1, step)
    return east, north, mass, rot


def stencil_of(east, north, mass, rot, keep, step):
    west = shift(east, -step, 0)
    south = shift(north, -step, 1)
    diag = mass + east + west + north + south
    return east, west, north, south, diag, keep * (RELAX / diag), rot


def off_diagonal(w, st, step):
    east, west, north, south, _, _, rot = st
    out = []
    for c in range(2):
        turned = -w[1] if c == 0 else w[0]
        out.append(
            east * shift(w[c], step, 0)
            + west * shift(w[c], -step, 0)
            + north * shift(w[c], step, 1)
            + south * shift(w[c], -step, 1)
            - rot * turned
        )
    return out


def from_zero(b, st):
    return [st[5] * b[c] for c in range(2)]


def residual_from_zero(b, w, st, step):
    off = off_diagonal(w, st, step)
    return [(1.0 - RELAX) * b[c] + off[c] for c in range(2)]


def sweep(w, b, st, step):
    off = off_diagonal(w, st, step)
    return [w[c] + st[5] * (b[c] - st[4] * w[c] + off[c]) for c in range(2)]


def restrict(r, step):
    return [0.25 * pair_sum(pair_sum(r[c], 0, step), 1, step) for c in range(2)]


def halo_place(k):
    return jnp.where(k < HALF, k // COMP, k // COMP + LANES - LANES // COMP)


def compact(x, own, select):
    block = COMP * LANES
    row, col = iota((block, LANES), 0), iota((block, LANES), 1)
    hit = (row == COMP * col + COMP - 1) if select else (row // COMP == col)
    m = jnp.where(hit, 1.0 / COMP, 0.0)
    row, col = iota((LANES, LANES), 0), iota((LANES, LANES), 1)
    hit = halo_place(row) == col
    if select:
        hit = hit & (row % COMP == COMP - 1)
    mh = jnp.where(hit, 1.0 / COMP, 0.0)
    out = [
        pick_right(x[:, k * block : (k + 1) * block], m)
        for k in range(own // block)
    ]
    out.append(pick_right(x[:, own:], mh))
    return jnp.concatenate(out, 1)


def expand(x, own):
    block = COMP * LANES
    row, col = iota((LANES, block), 0), iota((LANES, block), 1)
    m = jnp.where(row == col // COMP, 1.0, 0.0)
    row, col = iota((LANES, LANES), 0), iota((LANES, LANES), 1)
    mh = jnp.where(row == halo_place(col), 1.0, 0.0)
    count = own // block
    out = [
        pick_right(x[:, k * LANES : (k + 1) * LANES], m)
        for k in range(count)
    ]
    out.append(pick_right(x[:, count * LANES :], mh))
    return jnp.concatenate(out, 1)


DEPTH = (6, 5, 5, 5)
FILL = (0.0, 1.0, 0.0, 0.0)


def edges():
    offset, out = 0, []
    for depth in DEPTH:
        out.append((offset, depth))
        offset += depth
    return out


def kernel(
    gx, gy, f_hbm, v_hbm, m_hbm, cor_ref, land_hbm, ice_ref, out_ref,
    f_ref, v_ref, m_ref, land_ref, ext, rotx, low_pack, top_pack, from_n, from_s,
    to_r, to_l, from_r, from_l, lev2, load, send, recv,
):
    nx, ny = v_ref.shape
    full = ny + LANES
    grp = lax.axis_index("groups")
    g = lax.axis_index("gx")
    r = lax.axis_index("gy")
    at_top = r == gy - 1
    at_bottom = r == 0
    not_top = jnp.logical_not(at_top)
    not_bottom = jnp.logical_not(at_bottom)
    right = (grp, lax.rem(g + 1, gx), r)
    left = (grp, lax.rem(g + gx - 1, gx), r)
    above = (grp, g, r + 1)
    below = (grp, g, r - 1)
    mirror = (grp, gx - 1 - g, r)

    barrier = pltpu.get_barrier_semaphore()

    def hello(device):
        pl.semaphore_signal(barrier, inc=1, device_id=device, device_id_type=MESH)

    @pl.when(at_top)
    def _():
        hello(mirror)

    hello(right)
    hello(left)

    @pl.when(not_top)
    def _():
        hello(above)

    @pl.when(not_bottom)
    def _():
        hello(below)

    loads = [
        pltpu.make_async_copy(a, b, load.at[k])
        for k, (a, b) in enumerate(((land_hbm, land_ref), (v_hbm, v_ref), (m_hbm, m_ref), (f_hbm, f_ref)))
    ]
    for c in loads:
        c.start()
    tiles_x, tiles_y = ice_ref.shape
    ice_f = ice_ref[...].astype(jnp.float32)
    tile_row = (g * nx + iota((nx, tiles_y), 0)) // TILE
    ice_rows = jnp.zeros((nx, tiles_y), jnp.float32)
    for t in range(tiles_x):
        ice_rows = ice_rows + jnp.where(tile_row == t, ice_f[t : t + 1, :], 0.0)
    pick = jnp.where((r * ny + iota((tiles_y, ny), 1)) // TILE == iota((tiles_y, ny), 0), 1.0, 0.0)
    ice = jnp.dot(ice_rows, pick, preferred_element_type=jnp.float32)
    rotx[:, 0:ny] = jnp.broadcast_to(cor_ref[...].reshape(1, ny), (8, ny))
    for f in range(4):
        ext[f, nx:, :] = jnp.full((2 * HX, full), FILL[f], jnp.float32)
    for c in loads:
        c.wait()
    land = land_ref[...].astype(jnp.float32)
    ocean = 1.0 - land
    ext[0, 0:nx, 0:ny] = v_ref[...] * ice * ocean
    ext[1, 0:nx, 0:ny] = m_ref[...] * ocean + LAND_MASS * land
    ext[2, 0:nx, 0:ny] = f_ref[0] * ocean
    ext[3, 0:nx, 0:ny] = f_ref[1] * ocean

    group = iota((nx, LANES), 1) // HALF
    low, top = jnp.zeros((nx, LANES), jnp.float32), jnp.zeros((nx, LANES), jnp.float32)
    for f in range(4):
        low = jnp.where(group == f, pltpu.roll(ext[f, 0:nx, 0:LANES], HALF * f, 1), low)
        top = jnp.where(
            group == f, pltpu.roll(ext[f, 0:nx, ny - LANES : ny], (HALF * (f + 1)) % LANES, 1), top)
    low_pack[0:nx] = low
    low_pack[nx:] = rotx[:, 0:LANES]
    top_pack[0:nx] = top
    top_pack[nx:] = pltpu.roll(rotx[:, ny - LANES : ny], HALF, 1)

    for f, (o, d) in enumerate(edges()):
        to_r[o : o + d, 0:ny] = ext[f, nx - d : nx, 0:ny]
        to_l[o : o + d, 0:ny] = ext[f, 0:d, 0:ny]

    pl.semaphore_wait(barrier, jnp.where(at_bottom, 3, 4))

    def copy(src, dst, k, device):
        return pltpu.make_async_remote_copy(
            src_ref=src, dst_ref=dst, send_sem=send.at[k], recv_sem=recv.at[k],
            device_id=device, device_id_type=MESH,
        )

    to_mirror = copy(top_pack, from_n, 0, mirror)
    to_above = copy(top_pack, from_s, 1, above)
    to_below = copy(low_pack, from_n, 2, below)

    @pl.when(at_top)
    def _():
        to_mirror.start()

    @pl.when(not_top)
    def _():
        to_above.start()

    @pl.when(not_bottom)
    def _():
        to_below.start()

    def strips(k, lo, hi):
        return (
            copy(to_r.at[:, lo:hi], from_l.at[:, lo:hi], k, right),
            copy(to_l.at[:, lo:hi], from_r.at[:, lo:hi], k + 1, left),
        )

    bulk = strips(3, 0, ny)
    for c in bulk:
        c.start()

    @pl.when(at_top)
    def _():
        to_mirror.wait()
        row, col = iota((LANES, LANES), 0), iota((LANES, LANES), 1)
        flip_l = jnp.where((row // HALF == col // HALF) & (row % HALF + col % HALF == HALF - 1), 1.0, 0.0)
        row, col = iota((nx, nx), 0), iota((nx, nx), 1)
        flip_r = jnp.where(row + col == nx - 1, 1.0, 0.0)
        t = pick_right(from_n[...], flip_l)
        from_n[0:nx] = pick_left(flip_r, t[0:nx]) * jnp.where(group >= 2, -1.0, 1.0)
        from_n[nx:] = t[nx:]

    @pl.when(not_top)
    def _():
        to_above.wait_send()
        to_below.wait_recv()

    @pl.when(not_bottom)
    def _():
        to_below.wait_send()
        to_above.wait_recv()

    @pl.when(at_bottom)
    def _():
        from_s[...] = jnp.zeros(from_s.shape, jnp.float32)
        from_s[0:nx] = jnp.where(
            group == 0, jnp.broadcast_to(ext[0, 0:nx, 0:1], (nx, LANES)), jnp.where(group == 1, 1.0, 0.0))

    for f in range(4):
        n = pltpu.roll(from_n[0:nx], (LANES - HALF * f) % LANES, 1)
        s = pltpu.roll(from_s[0:nx], (LANES - HALF * (f + 1)) % LANES, 1)
        ext[f, 0:nx, ny:full] = jnp.where(group == 0, n, jnp.where(group == LANES // HALF - 1, s, FILL[f]))
    group8 = iota((8, LANES), 1) // HALF
    rotx[:, ny:full] = jnp.where(group8 == 0, from_n[nx:], pltpu.roll(from_s[nx:], LANES - HALF, 1))
    for f, (o, d) in enumerate(edges()):
        to_r[o : o + d, ny:full] = ext[f, nx - d : nx, ny:full]
        to_l[o : o + d, ny:full] = ext[f, 0:d, ny:full]

    corner = strips(5, ny, full)
    for c in corner:
        c.start()
    own_v, own_m, rot = ext[0, 0:nx], ext[1, 0:nx], rotx[...]
    own_e = 0.5 * (own_v + shift(own_v, 1, 0))
    own_n = 0.5 * (own_v + shift(own_v, 1, 1))
    cx = nx // COMP
    row, col = iota((cx, nx), 0), iota((cx, nx), 1)
    mean_rows = jnp.where(col // COMP == row, 1.0 / COMP, 0.0)
    last_rows = jnp.where(col == COMP * row + COMP - 1, 1.0 / COMP, 0.0)
    avg = compact(jnp.concatenate([own_m, own_e, rot], 0), ny, False)
    lev2[2, 0:cx] = pick_left(mean_rows, avg[0:nx])
    lev2[3, 0:cx] = pick_left(last_rows, avg[nx : 2 * nx])
    lev2[4, 0:cx] = pick_left(mean_rows, compact(own_n, ny, True))
    rot2 = avg[2 * nx : 2 * nx + 8]

    def blocks(k, lo, hi):
        return (
            copy(lev2.at[lo:hi, 0:cx], lev2.at[lo:hi, 2 * cx : 3 * cx], k, right),
            copy(lev2.at[lo:hi, 0:cx], lev2.at[lo:hi, cx : 2 * cx], k + 1, left),
        )

    first = blocks(7, 2, 5)
    for c in bulk:
        c.wait()
    for c in corner:
        c.wait()
    for c in first:
        c.start()
    for f, (o, d) in enumerate(edges()):
        ext[f, nx : nx + d] = from_r[o : o + d]
        ext[f, nx + 2 * HX - d : nx + 2 * HX] = from_l[o : o + d]

    visc, mass = ext[0], ext[1]
    src = [ext[2], ext[3]]
    lane = iota((1, full), 1)
    used = (lane < ny + HALF) | ((lane >= full - HALF) & not_bottom)
    keep = jnp.where(used, 1.0, 0.0)
    east = 0.5 * (visc + shift(visc, 1, 0))
    north = 0.5 * (visc + shift(visc, 1, 1))
    face = compact(
        jnp.concatenate([0.5 * (visc[nx - 1 : nx] + visc[nx : nx + 1]),
                         0.5 * (visc[nx + 2 * HX - 1 : nx + 2 * HX] + visc[0:1])] * 4, 0), ny, False)
    face = (1.0 / COMP) * face
    st0 = stencil_of(east, north, mass, rot[0:1], keep, 1)
    w0 = from_zero(src, st0)
    b1 = restrict(residual_from_zero(src, w0, st0, 1), 1)
    east1, north1, mass1, rot1 = coarsen(east, north, mass, rot, 1)
    st1 = stencil_of(east1, north1, mass1, rot1[0:1], keep, 2)
    w1 = from_zero(b1, st1)
    r1 = residual_from_zero(b1, w1, st1, 2)
    avg = compact(jnp.concatenate([r1[0][0:nx], r1[1][0:nx]], 0), ny, False)
    for k in range(2):
        lev2[k, 0:cx] = pick_left(mean_rows, avg[k * nx : (k + 1) * nx])
    second = blocks(9, 0, 2)
    for c in second:
        c.start()
    for c in first:
        c.wait()
    mass2, east2, north2 = lev2[2], lev2[3], lev2[4]
    row2 = iota(east2.shape, 0)
    east2 = jnp.where(row2 == cx - 1, face[0:1], jnp.where(row2 == 3 * cx - 1, face[1:2], east2))
    full2 = lev2.shape[2]
    lane2 = iota((1, full2), 1)
    used = (lane2 < ny // COMP + HALF // COMP) | (lane2 >= full2 - HALF // COMP)
    below2 = (lane2 >= full2 - HALF // COMP) & at_bottom
    keep2 = jnp.where(used & jnp.logical_not(below2), 1.0, 0.0)
    mass2 = jnp.where(used, mass2, 1.0)
    st2 = stencil_of(east2, north2, mass2, rot2[0:1], keep2, 1)
    east3, north3, mass3, rot3 = coarsen(east2, north2, mass2, rot2, 1)
    st3 = stencil_of(east3, north3, mass3, rot3[0:1], keep2, 2)
    for c in second:
        c.wait()
    b2 = [lev2[0], lev2[1]]
    w2 = from_zero(b2, st2)
    b3 = restrict(residual_from_zero(b2, w2, st2, 1), 1)
    e3 = from_zero(b3, st3)
    e3 = sweep(e3, b3, st3, 2)
    e3 = sweep(e3, b3, st3, 2)
    w2 = sweep([w2[c] + e3[c] for c in range(2)], b2, st2, 1)
    row, col = iota((nx + 2 * HX, 3 * cx), 0), iota((nx + 2 * HX, 3 * cx), 1)
    from_row = jnp.where(row < nx + HX, row // COMP, row // COMP + 3 * cx - (nx + 2 * HX) // COMP)
    spread = jnp.where(from_row == col, 1.0, 0.0)
    up = expand(jnp.concatenate([pick_left(spread, w2[c]) for c in range(2)], 0), ny)
    up = [up[0 : nx + 2 * HX], up[nx + 2 * HX :]]
    e1 = sweep([w1[c] + up[c] for c in range(2)], b1, st1, 2)
    def crop(x):
        return x[0:nx, 0:ny]

    w0 = [w0[c] + e1[c] for c in range(2)]
    east, west, north, south, diag, inverse = [crop(x) for x in st0[:6]]
    for c in range(2):
        w, turned = w0[c], crop(-w0[1] if c == 0 else w0[0])
        out_ref[c] = crop(w) + inverse * (
            crop(src[c]) - diag * crop(w) + east * crop(shift(w, 1, 0)) + west * crop(shift(w, -1, 0))
            + north * crop(shift(w, 1, 1)) + south * crop(shift(w, -1, 1)) - rot[0:1, 0:ny] * turned)


def local(gx, gy, forcing, viscosity, mass, coriolis, land, ice_tiles):
    nx, ny = viscosity.shape
    ext = (nx + 2 * HX, ny + LANES)
    strip = pltpu.VMEM((nx + 8, LANES), jnp.float32)
    height = -(-sum(DEPTH) // 8) * 8
    side = pltpu.VMEM((height, ny + LANES), jnp.float32)
    anyspace = pl.BlockSpec(memory_space=pl.ANY)
    vmem = pl.BlockSpec(memory_space=pltpu.VMEM)
    return pl.pallas_call(
        functools.partial(kernel, gx, gy),
        out_shape=jax.ShapeDtypeStruct(forcing.shape, jnp.float32),
        in_specs=[anyspace, anyspace, anyspace, vmem, anyspace, vmem],
        out_specs=vmem,
        scratch_shapes=[
            pltpu.VMEM(forcing.shape, jnp.float32),
            pltpu.VMEM((nx, ny), jnp.float32),
            pltpu.VMEM((nx, ny), jnp.float32),
            pltpu.VMEM((nx, ny), jnp.int32),
            pltpu.VMEM((4,) + ext, jnp.float32),
            pltpu.VMEM((8, ny + LANES), jnp.float32),
            strip, strip, strip, strip,
            side, side, side, side,
            pltpu.VMEM((5, 3 * (nx // COMP), ny // COMP + LANES), jnp.float32),
            pltpu.SemaphoreType.DMA((4,)),
            pltpu.SemaphoreType.DMA((11,)),
            pltpu.SemaphoreType.DMA((11,)),
        ],
        compiler_params=pltpu.CompilerParams(collective_id=0, has_side_effects=True),
    )(forcing, viscosity, mass, coriolis, land, ice_tiles)


def solution(mesh):
    return jax.shard_map(
        functools.partial(local, mesh.shape["gx"], mesh.shape["gy"]),
        mesh=mesh,
        in_specs=(
            P(None, ("groups", "gx"), "gy"),
            P(("groups", "gx"), "gy"),
            P(("groups", "gx"), "gy"),
            P("gy"),
            P("gx", "gy"),
            P("groups", None),
        ),
        out_specs=P(None, ("groups", "gx"), "gy"),
        check_vma=False,
    )
```
